256 devices in a mesh: lat: 16 (over z, core), lon: 16 (over y, x).
Axes of the slice: x: 4, y: 4, z: 8, core: 2. Of those that a mesh axis runs over, the one named last changes fastest.
Arguments:
- predicted_state: float32 [1440, 26624], P('lon', 'lat'), may hold values from -24 to 24
- verified_state: float32 [1440, 26624], P('lon', 'lat'), may hold values from -20 to 20
- normal_state: float32 [1440, 26624], P('lon', 'lat'), may hold values from -3 to 3
Outputs:
- energy_curves: float32 [3, 52, 721], replicated
- rms_error: float32 [52], replicated
- anomaly_corr: float32 [52], replicated
The draws below stay inside these ranges and needn't reach their ends.
All inputs are finite; a program needn't handle non-finite values.
Results may differ from the reference program's by a relative error of at most 0.00005.
Values sent between devices are 32-bit elements; how exact they have to be, the bound alone decides.
No kernel may reach another device: no remote copies, remote signals or barrier semaphores. Data moves between devices by JAX's collectives and lax.ppermute only.
A program may use at most 64 MiB of HBM per device.

```python
import jax
import jax.numpy as jnp
from jax import lax

VARS = 4
LEVELS = 13
NLON = 1440
FIELDS = 52
NLAT = 512


def noise_field(key):
    array_extent = (VARS * LEVELS, NLAT, NLON)
    lat_scale = 3.0 ** (jnp.arange(NLAT).astype(jnp.float32) / max(NLAT - 1, 1))
    base = jax.random.truncated_normal(key, -4.0, 4.0, array_extent, jnp.float32)
    full = base * lat_scale[None, :, None]
    return full.transpose(2, 1, 0).reshape(NLON, NLAT * VARS * LEVELS)


def draw_verified_state(key, part):
    return noise_field(jax.random.fold_in(key, 101))


def draw_predicted_state(key, part):
    shared = noise_field(jax.random.fold_in(key, 101))
    extra = noise_field(jax.random.fold_in(key, 202))
    return 0.8 * shared + 0.6 * extra


def steps_of(rng, dims, cuts, least, top_value):
    def one(axis_at, parts):
        draws = jax.random.uniform(jax.random.fold_in(jax.random.fold_in(rng, 6), axis_at), (parts,), jnp.float32, least / len(cuts), top_value / len(cuts))
        return jnp.repeat(jnp.exp(draws), dims[axis_at] // parts).reshape((-1,) + (1,) * (len(dims) - axis_at - 1))

    loudness = one(*cuts[0])
    for cut in cuts[1:]:
        loudness = loudness * one(*cut)
    return loudness


def noise(stream_key, dims, scale, limit, split=(), held_as=jnp.bfloat16):
    values = jax.random.normal(stream_key, dims, jnp.float32) * scale
    if len(split) > 0:
        values = steps_of(stream_key, dims, split, -0.22, 0.18) * values
    return jnp.clip(values, min=-limit, max=limit).astype(held_as)


def setup_inputs(seed: int = 0) -> dict:
    splits = jax.random.split(jax.random.key(seed), 4)
    return {
        "predicted_state": draw_predicted_state(jax.random.fold_in(splits[3], 71), 0),
        "verified_state": draw_verified_state(jax.random.fold_in(splits[3], 71), 0),
        "normal_state": noise(splits[2], (NLON, NLAT * FIELDS), 0.5, 3.0, ((0, 16), (1, 16)), jnp.float32),
    }


def latitude_weights(parallel_number):
    index = jnp.arange(parallel_number).astype(jnp.float32)
    return jnp.cos(jnp.pi * ((index + 0.5) / parallel_number - 0.5))

def separate_quantities(packed):
    return packed.reshape(NLON, NLAT, FIELDS).transpose(2, 1, 0)

def reference(predicted_state, verified_state, normal_state):
    predicted_state = separate_quantities(predicted_state)
    verified_state = separate_quantities(verified_state)
    normal_state = separate_quantities(normal_state)
    parallel_number = predicted_state.shape[1]
    weights = latitude_weights(parallel_number)
    weight_total = jnp.sum(weights)
    mismatch_parts = predicted_state - verified_state

    def energy_by_wavenumber(field):
        coeffs = jnp.fft.rfft(field, axis=2)
        powers = coeffs.real * coeffs.real + coeffs.imag * coeffs.imag
        return lax.optimization_barrier(jnp.sum(weights[None, :, None] * powers, axis=1)) / (NLON * NLON * weight_total)
    energy_curves = jnp.stack([energy_by_wavenumber(predicted_state), energy_by_wavenumber(verified_state), energy_by_wavenumber(mismatch_parts)])
    predicted_anomalies = predicted_state - normal_state
    observed_anomalies = verified_state - normal_state
    broad_layout = weights[None, :, None]
    normalizer = NLON * weight_total
    m_ee = lax.optimization_barrier(jnp.sum(broad_layout * mismatch_parts * mismatch_parts, axis=(1, 2))) / normalizer
    cross_moment = lax.optimization_barrier(jnp.sum(broad_layout * predicted_anomalies * observed_anomalies, axis=(1, 2))) / normalizer
    predicted_moment = lax.optimization_barrier(jnp.sum(broad_layout * predicted_anomalies * predicted_anomalies, axis=(1, 2))) / normalizer
    m_tt = lax.optimization_barrier(jnp.sum(broad_layout * observed_anomalies * observed_anomalies, axis=(1, 2))) / normalizer
    rms_error = jnp.sqrt(m_ee)
    anomaly_corr = cross_moment / jnp.sqrt((predicted_moment + 1e-06) * (m_tt + 1e-06))
    return (energy_curves, rms_error, anomaly_corr)
```

```python
import functools

import jax
import jax.numpy as jnp
import numpy as np
from jax import lax
from jax.experimental import pallas as pl
from jax.experimental.pallas import tpu as pltpu
from jax.sharding import Mesh
from jax.sharding import PartitionSpec as P

FIELDS = 52
NLON = 1440
NLAT = 512
BLOCKS = 16
BLOCK = NLON // BLOCKS
WAVES = NLON // 2 + 1
LAT_LINES = 32
COLS = FIELDS * LAT_LINES
SHARE = COLS // BLOCKS
WHOLE = 3
REST = 8
HEAD = 64
TAIL_ROWS = 56
ROWS = SHARE + TAIL_ROWS
LANES = 128
WIDE = 768
HALF = WIDE // 2
LAT = ("lat_0", "lat_1")
LON = ("lon_0", "lon_1")

epsilon = 1e-06


def out_wave(k0, lane):
    if k0 == 0:
        if lane < 46:
            return 16 * lane
        if lane < 91:
            return 8 + 16 * (lane - 46)
        return -1
    if lane < 90:
        k = k0 + 16 * lane
        return min(k, NLON - k)
    return -1


def dft_tables():
    table = np.zeros((8, 256, 256), np.float64)
    m = np.arange(BLOCK)
    re_row = np.where(m < HEAD, m, 128 + m - HEAD)
    im_row = np.where(m < HEAD, HEAD + m, 160 + m - HEAD)
    for lane in range(90):
        for k0 in range(1, 8):
            angle = 2.0 * np.pi * ((m * (k0 + 16 * lane)) % NLON) / NLON
            table[k0, re_row, lane] = np.cos(angle)
            table[k0, im_row, lane] = np.sin(angle)
            table[k0, re_row, 128 + lane] = -np.sin(angle)
            table[k0, im_row, 128 + lane] = np.cos(angle)
    for lane in range(91):
        angle = 2.0 * np.pi * ((m * out_wave(0, lane)) % NLON) / NLON
        rows = re_row if lane < 46 else im_row
        table[0, rows, lane] = np.cos(angle)
        table[0, rows, 128 + lane] = -np.sin(angle)
    full = table.astype(np.float32)
    high = full.astype(jnp.bfloat16)
    low = (table - high.astype(np.float64)).astype(np.float32).astype(jnp.bfloat16)
    return np.concatenate([high, low], axis=0)


def order_table():
    row = jnp.arange(8 * LANES, dtype=jnp.int32)
    k0, lane = row // LANES, row % LANES
    ahead = k0 + 16 * lane
    wave = jnp.where(lane < 90, jnp.minimum(ahead, NLON - ahead), -1)
    first = jnp.where(lane < 46, 16 * lane, jnp.where(lane < 91, 8 + 16 * (lane - 46), -1))
    wave = jnp.where(k0 == 0, first, wave)
    return (wave[:, None] == jnp.arange(WIDE, dtype=jnp.int32)[None, :]).astype(jnp.bfloat16)


def pack_kernel(fore_ref, true_ref, out_ref, head_ref, tail_ref):
    lane = lax.broadcasted_iota(jnp.int32, (8, LANES), 1)
    pad = jnp.zeros((96 - BLOCK, LANES), jnp.float32)
    for j in range(COLS // LANES):
        cols = slice(j * LANES, (j + 1) * LANES)
        head = jnp.concatenate([fore_ref[:HEAD, cols], true_ref[:HEAD, cols]], axis=0)
        head_ref[cols, :] = head.T
        tail = jnp.concatenate(
            [fore_ref[HEAD:, cols], pad, true_ref[HEAD:, cols], pad], axis=0
        )
        tail = jnp.concatenate([tail, tail], axis=0)
        tail_ref[cols, :] = tail.T

    def piece(ref, s, part):
        if part < 12:
            field = WHOLE * s + part // 4
            first = 8 * (part % 4)
        else:
            field = WHOLE * BLOCKS + s // 4
            first = 8 * (s % 4)
        return ref[pl.ds(first * FIELDS + field, 8, stride=FIELDS), :]

    for s in range(BLOCKS):
        for part in range(13):
            out_ref[s, 8 * part : 8 * part + 8, :] = piece(head_ref, s, part)
        for part in range(7):
            near = piece(tail_ref, s, part)
            far = piece(tail_ref, s, min(part + 7, 12))
            out_ref[s, SHARE + 8 * part : SHARE + 8 * part + 8, :] = jnp.where(lane < HEAD, near, far)


def pack(fore, true):
    return pl.pallas_call(
        pack_kernel,
        out_shape=jax.ShapeDtypeStruct((BLOCKS, ROWS, LANES), jnp.float32),
        in_specs=[pl.BlockSpec(memory_space=pltpu.VMEM)] * 2,
        out_specs=pl.BlockSpec(memory_space=pltpu.VMEM),
        scratch_shapes=[pltpu.VMEM((COLS, LANES), jnp.float32)] * 2,
        name="pack",
    )(fore, true)


def sixteen(x):
    half = float(np.sqrt(0.5))
    e = [x[j] + x[j + 8] for j in range(8)]
    o = [x[j] - x[j + 8] for j in range(8)]
    ee = [e[j] + e[j + 4] for j in range(4)]
    eo = [e[j] - e[j + 4] for j in range(4)]
    a, b = ee[0] + ee[2], ee[1] + ee[3]
    out = {0: (a + b, a - b), 4: (ee[0] - ee[2], ee[3] - ee[1])}
    s, d = half * (eo[1] + eo[3]), half * (eo[1] - eo[3])
    out[2] = (eo[0] + d, -(eo[2] + s))
    out[6] = (eo[0] - d, eo[2] - s)
    p = [o[j] - o[8 - j] for j in range(1, 4)]
    q = [o[j] + o[8 - j] for j in range(1, 4)]
    for k in (1, 3, 5, 7):
        re, im = o[0], -float(np.round(np.sin(np.pi * k / 2))) * o[4]
        for j in range(1, 4):
            re = re + float(np.cos(np.pi * j * k / 8)) * p[j - 1]
            im = im - float(np.sin(np.pi * j * k / 8)) * q[j - 1]
        out[k] = (re, im)
    return out


def spectrum_kernel(got_ref, weight_ref, skill_ref, table_ref, order_ref, out_ref, y_ref, rows_ref):
    def butterfly(i, _):
        rows = pl.ds(pl.multiple_of(i * 8, 8), 8)
        out = sixteen([got_ref[d, rows, :] for d in range(BLOCKS)])
        for k0 in range(8):
            y_ref[2 * k0, rows, :] = out[k0][0]
            y_ref[2 * k0 + 1, rows, :] = out[k0][1]
        return 0

    lax.fori_loop(0, ROWS // 8, butterfly, 0, unroll=2)
    lane_head = lax.broadcasted_iota(jnp.int32, (SHARE, LANES), 1) < 64
    lane_tail = lax.broadcasted_iota(jnp.int32, (TAIL_ROWS, LANES), 1) < 32
    weight = weight_ref[...]
    for k0 in range(8):
        re, im = y_ref[2 * k0, :SHARE, :], y_ref[2 * k0 + 1, :SHARE, :]
        fore_head = jnp.where(lane_head, re, pltpu.roll(im, 64, 1))
        true_head = jnp.where(lane_head, pltpu.roll(re, 64, 1), im)
        re, im = y_ref[2 * k0, SHARE:, :], y_ref[2 * k0 + 1, SHARE:, :]
        slots = [
            jnp.where(
                lane_tail,
                re if s == 0 else pltpu.roll(re, 128 - 32 * s, 1),
                im if s == 1 else pltpu.roll(im, (160 - 32 * s) % 128, 1),
            )
            for s in range(4)
        ]
        rest = SHARE - TAIL_ROWS
        heads = jnp.concatenate([fore_head, true_head], axis=0)
        tails = jnp.concatenate([slots[0], slots[2][:rest], slots[1], slots[3][:rest]], axis=0)
        z = jnp.concatenate([heads, tails], axis=1)
        high = z.astype(jnp.bfloat16)
        low = (z - high.astype(jnp.float32)).astype(jnp.bfloat16)
        t_high, t_low = table_ref[k0], table_ref[8 + k0]
        dot = functools.partial(jnp.dot, preferred_element_type=jnp.float32)
        coeffs = dot(high, t_high) + (dot(low, t_high) + dot(high, t_low))
        fore, true = coeffs[:SHARE], coeffs[SHARE:]
        for c, part in enumerate((fore, true, fore - true)):
            square = part * part
            power = (square[:, :LANES] + square[:, LANES:]) * weight
            for f in range(4):
                first, last = 32 * f, min(32 * f + 32, SHARE)
                rows_ref[4 * c + f : 4 * c + f + 1, k0 * LANES : (k0 + 1) * LANES] = jnp.sum(
                    power[first:last], axis=0, keepdims=True
                )
    rows = rows_ref[:12, :]
    high = rows.astype(jnp.bfloat16)
    left = rows - high.astype(jnp.float32)
    middle = left.astype(jnp.bfloat16)
    low = (left - middle.astype(jnp.float32)).astype(jnp.bfloat16)
    order = order_ref[...]
    dot = functools.partial(jnp.dot, preferred_element_type=jnp.float32)
    placed = dot(high, order) + (dot(middle, order) + dot(low, order))
    out_ref[0, :12, :] = placed[:, :HALF]
    out_ref[1, :12, :] = placed[:, HALF:]
    out_ref[0, 12:, :] = skill_ref[...]
    out_ref[1, 12:, :] = jnp.zeros((4, HALF), jnp.float32)


def spectrum(got, weight, skill, table, order):
    return pl.pallas_call(
        spectrum_kernel,
        out_shape=jax.ShapeDtypeStruct((2, 16, HALF), jnp.float32),
        in_specs=[pl.BlockSpec(memory_space=pltpu.VMEM)] * 5,
        out_specs=pl.BlockSpec(memory_space=pltpu.VMEM),
        scratch_shapes=[
            pltpu.VMEM((BLOCKS, ROWS, LANES), jnp.float32),
            pltpu.VMEM((16, 8 * LANES), jnp.float32),
        ],
        name="spectrum",
    )(got, weight, skill, table, order)


def latitude_weights(lat_index):
    return jnp.cos(jnp.pi * ((lat_index.astype(jnp.float32) + 0.5) / NLAT - 0.5))


def to_all(value, axis):
    copies = jnp.broadcast_to(value, (lax.axis_size(axis), *value.shape))
    return lax.all_to_all(copies, axis, split_axis=0, concat_axis=0, tiled=True)


def skill_sums(predicted_state, verified_state, normal_state, weights):
    predicted = predicted_state - normal_state
    observed = verified_state - normal_state
    mismatch = predicted_state - verified_state
    column = jnp.repeat(weights, FIELDS)
    terms = [
        jnp.sum(u * v, axis=0) * column
        for u, v in (
            (mismatch, mismatch),
            (predicted, observed),
            (predicted, predicted),
            (observed, observed),
        )
    ]
    return jnp.stack([t.reshape(LAT_LINES, FIELDS).sum(axis=0) for t in terms])


def local(predicted_state, verified_state, normal_state):
    lon = lax.axis_index(LON)
    core = lax.axis_index("lat_1")
    lat_first = lax.axis_index(LAT) * LAT_LINES
    swap = [(0, 1), (1, 0)]
    message = pack(predicted_state, verified_state)
    got = lax.all_to_all(message, LON, split_axis=0, concat_axis=0, tiled=True)

    weights = latitude_weights(lat_first + jnp.arange(LAT_LINES, dtype=jnp.int32))
    weight_total = jnp.sum(latitude_weights(jnp.arange(NLAT, dtype=jnp.int32)))
    row = jnp.arange(SHARE, dtype=jnp.int32)
    row_lat = jnp.where(row < WHOLE * LAT_LINES, row % LAT_LINES, 8 * (lon % 4) + row % 8)
    row_weight = latitude_weights(lat_first + row_lat) / (NLON * NLON * weight_total)
    row_weight = jnp.broadcast_to(row_weight[:, None], (SHARE, LANES))
    skill = skill_sums(predicted_state, verified_state, normal_state, weights)
    skill = jnp.pad(skill, ((0, 0), (0, HALF - FIELDS)))

    parts = spectrum(got, row_weight, skill, jnp.asarray(dft_tables()), order_table())
    mine = jnp.where(core == 0, parts[0], parts[1])
    theirs = jnp.where(core == 0, parts[1], parts[0])
    half = mine + lax.ppermute(theirs, "lat_1", swap)
    half = to_all(half, "lat_0").sum(axis=0)
    shares = to_all(half, LON)

    groups = shares[:, :12].reshape(BLOCKS, 3, 4, HALF).transpose(1, 0, 2, 3)
    whole = groups[:, :, :WHOLE].reshape(3, WHOLE * BLOCKS, HALF)
    rest = groups[:, :, WHOLE].reshape(3, 4, 4, HALF).sum(axis=2)
    sums = shares[:, 12:].sum(axis=0)
    mine = jnp.concatenate(
        [whole.reshape(-1, HALF), rest.reshape(-1, HALF), sums], axis=0
    )
    theirs = lax.ppermute(mine, "lat_1", swap)
    first = jnp.where(core == 0, mine, theirs)
    second = jnp.where(core == 0, theirs, mine)
    both = jnp.concatenate([first, second], axis=1)
    split = 3 * WHOLE * BLOCKS
    energy_curves = jnp.concatenate(
        [both[:split].reshape(3, -1, WIDE), both[split : split + 12].reshape(3, 4, WIDE)], axis=1
    )[:, :, :WAVES]
    means = first[split + 12 :, :FIELDS] / (NLON * weight_total)
    rms_error = jnp.sqrt(means[0])
    anomaly_corr = means[1] / jnp.sqrt((means[2] + epsilon) * (means[3] + epsilon))
    return energy_curves, rms_error, anomaly_corr


def solution(mesh):
    split = Mesh(mesh.devices.reshape(8, 2, 4, 4), ("lat_0", "lat_1", "lon_0", "lon_1"))
    placed = (P(LON, LAT), P(LON, LAT), P(LON, LAT))
    return jax.shard_map(
        local, mesh=split, in_specs=placed, out_specs=(P(), P(), P()), check_vma=False
    )
```
